32 devices in a mesh: row: 8 (over y, x, core), col: 4 (over z).
Axes of the slice: x: 2, y: 2, z: 4, core: 2. Of those that a mesh axis runs over, the one named last changes fastest.
Arguments:
- temps: bfloat16 [12, 64, 16384], P(None, None, ('row', 'col')), may hold values from -6 to 6
- sensors: int32 [12, 512], replicated, may hold values from 0 to 16383
Outputs:
- corr: bfloat16 [512, 16384], P('col', 'row')
The draws below stay inside these ranges and needn't reach their ends.
Inputs may be any that keep to these rules, and one draw needn't show every extreme that they name: `sensors`: each entry is a pixel index of its tier; candidates may repeat.
All inputs are finite; a program needn't handle non-finite values.
Results may differ from the reference program's by a relative error of at most 0.001.
Values may be sent and summed in bfloat16 or wider, within the bound.
A program may use at most 64 MiB of HBM per device.

```python
import jax
import jax.numpy as jnp
from jax import lax

TIERS = 12
SNAP = 64
PIX_DEV = 512
PIX = 16384
SENS = 512
N_ROW = 8
N_COL = 4


def with_ends(values, stream_key, low, top_value):
    longest = values.shape.index(max(values.shape))
    spots = []
    for shift in (0, 1):
        where = [jax.random.randint(jax.random.fold_in(stream_key, axis), (), 0, length) for axis, length in enumerate(values.shape)]
        where[longest] = (where[longest] + shift) % values.shape[longest]
        spots.append(tuple(where))
    return values.at[spots[0]].set(low).at[spots[1]].set(top_value)


def block_levels(own_key, dims, cuts, low, largest):
    def one(axis_at, parts):
        heights = jax.random.uniform(jax.random.fold_in(jax.random.fold_in(own_key, 6), axis_at), (parts,), jnp.float32, low / len(cuts), largest / len(cuts))
        return jnp.repeat(jnp.exp(heights), dims[axis_at] // parts).reshape((-1,) + (1,) * (len(dims) - axis_at - 1))

    loudness = one(*cuts[0])
    for cut in cuts[1:]:
        loudness = loudness * one(*cut)
    return loudness


def centred(own_key, shape, spread, reach, cuts=(), kind=jnp.bfloat16):
    array = jax.random.normal(own_key, shape, jnp.float32) * spread
    if len(cuts) > 0:
        array = block_levels(own_key, shape, cuts, -0.22, 0.18) * array
    return jnp.clip(array, min=-reach, max=reach).astype(kind)


def setup_inputs(seed: int = 0) -> dict:
    keys = jax.random.split(jax.random.key(seed), 3)
    return {
        "temps": centred(keys[0], (TIERS, SNAP, PIX), 1.0, 6.0, ((2, 32),)),
        "sensors": with_ends(jax.random.randint(keys[1], (TIERS, SENS), 0, PIX), jax.random.fold_in(keys[1], 1), 0, PIX - 1).astype(jnp.int32),
    }


def reference(temps, sensors):
    readings = jax.vmap(lambda fields, cols: jnp.take(fields, cols, axis=1))(temps, sensors)
    chosen = readings.astype(jnp.float32)
    block_width = PIX_DEV * N_COL
    scale_factor = 1.0 / jnp.sqrt(jnp.float32(TIERS * SNAP))

    def one_block(block_index):
        first_pixel = (block_index * block_width).astype(jnp.int32)
        fields = lax.dynamic_slice_in_dim(temps, first_pixel, block_width, 2).astype(jnp.float32)
        summed = jnp.einsum('tsc,tsp->cp', chosen, fields)
        return (summed * scale_factor).astype(jnp.bfloat16)
    blocks = lax.map(one_block, jnp.arange(N_ROW, dtype=jnp.int32))
    return jnp.transpose(blocks, (1, 0, 2)).reshape(SENS, PIX)
```

```python
import functools

import jax
import numpy as np
import jax.numpy as jnp
from jax import lax
from jax.experimental import pallas as pl
from jax.experimental.pallas import tpu as pltpu
from jax.sharding import PartitionSpec as P

SUB = 16
MESH = pl.DeviceIdType.MESH


def kernel(
    n_row, n_col, n_chunk, tiers,
    temps_hbm, sens_ref, out_ref,
    temps_ref, sens_t, part, core_buf, pair_sum, rs_buf, z_src, z_buf, full, out_buf,
    c_send, c_recv, rs_send, rs_recv, z_send, z_recv,
    ag_send, ag_recv, o_send, o_recv, t_sem, x_send, x_recv,
):
    r = lax.axis_index("row")
    z = lax.axis_index("col")
    core, chip = lax.rem(r, 2), r // 2
    other = 1 - core
    pair, parity = z // 2, lax.rem(z, 2)
    n_chip, n_pair = n_row // 2, n_col // 2
    depth, width = temps_ref.shape[1:]
    snaps, deep = depth // tiers, depth // 2
    rows_col = out_ref.shape[0] // n_chunk
    half = rows_col // 2
    rows_half = n_chip * SUB
    scale = float(np.float32(1.0) / np.sqrt(np.float32(depth)))
    partner = (chip * 2 + other, z)

    cube = [(d, e) for d in reversed(range(n_chip)) for e in (1, 0) if d or e]

    def cube_peer(d, e):
        peer = lax.rem(chip + d, n_chip)
        side = lax.rem(parity + e, 2)
        return side, peer, (peer * 2 + core, pair * 2 + side)

    def far_peer(e):
        return lax.rem(z + 2 * e, n_col)

    def column_peer(h, e):
        return (chip * 2 + lax.rem(core + h, 2), lax.rem(z + e, n_col))

    load = pltpu.make_async_copy(temps_hbm, temps_ref.at[core], t_sem)
    load.start()
    barrier = pltpu.get_barrier_semaphore()
    greeted = 0
    for d, e in cube:
        if d:
            pl.semaphore_signal(barrier, inc=1, device_id=cube_peer(d, e)[2], device_id_type=MESH)
            greeted += 1
    for h in range(2):
        for e in range(n_col):
            if h or e:
                pl.semaphore_signal(barrier, inc=1, device_id=column_peer(h, e), device_id_type=MESH)
                greeted += 1

    first_pixel = (r * n_col + z) * width
    offsets = jnp.transpose(sens_ref[...] - first_pixel)
    sens_t[...] = offsets.reshape(sens_t.shape)
    pixel_ids = lax.broadcasted_iota(jnp.int32, (rows_half, width), 1)

    def wait_all(ref, sem):
        pltpu.make_async_copy(ref, ref, sem).wait()

    def select(k):
        for h in range(2):
            mine = sens_t[:, k, h].reshape(rows_half, tiers)
            for t in range(0, tiers, 2):
                two = []
                for u in (t, t + 1):
                    hot = (pixel_ids == mine[:, u:u + 1]).astype(jnp.float32).astype(jnp.bfloat16)
                    two.append(lax.dot_general(
                        hot, temps_ref[core, u * snaps:(u + 1) * snaps, :],
                        (((1,), (1,)), ((), ())), preferred_element_type=jnp.float32,
                    ))
                both = jnp.concatenate(two, axis=1).astype(jnp.bfloat16)
                b, at = divmod(t * snaps, deep)
                part[k, h, b, :, :, at:at + 2 * snaps] = both.reshape(n_chip, SUB, 2 * snaps)

    def start_core(k):
        pltpu.make_async_remote_copy(
            part.at[k, other], core_buf.at[k], c_send.at[k], c_recv.at[k],
            device_id=partner, device_id_type=MESH,
        ).start()

    def start_rs(k):
        wait_all(core_buf.at[k], c_recv.at[k])
        pair_sum[k] = part[k, core] + core_buf[k]
        for slot, (d, e) in enumerate(cube):
            side, peer, device = cube_peer(d, e)
            pltpu.make_async_remote_copy(
                pair_sum.at[k, side, peer], rs_buf.at[k, slot], rs_send.at[k], rs_recv.at[k],
                device_id=device, device_id_type=MESH,
            ).start()

    def start_z(k):
        wait_all(rs_buf.at[k], rs_recv.at[k])
        total = pair_sum[k, parity, chip]
        for slot in range(len(cube)):
            total = total + rs_buf[k, slot]
        z_src[k] = total
        for e in range(1, n_pair):
            pltpu.make_async_remote_copy(
                z_src.at[k], z_buf.at[k, e - 1], z_send.at[k], z_recv.at[k],
                device_id=(r, far_peer(e)), device_id_type=MESH,
            ).start()

    def start_ag(k):
        wait_all(z_buf.at[k], z_recv.at[k])
        total = z_src[k]
        for e in range(n_pair - 1):
            total = total + z_buf[k, e]
        full[k, parity, chip] = total
        for d, e in cube:
            pltpu.make_async_remote_copy(
                full.at[k, parity, chip], full.at[k, parity, chip], ag_send.at[k], ag_recv.at[k],
                device_id=cube_peer(d, e)[2], device_id_type=MESH,
            ).start()

    n_half = n_col // 2
    side_z = z // n_half

    def out_peer(e):
        across = (1 - side_z) * n_half + lax.rem(z + e, n_half)
        beside = side_z * n_half + lax.rem(z + e, n_half)
        return across if e < n_half else beside

    def start_out(k):
        if k == 0:
            wait_all(temps_ref.at[other], x_recv)
        wait_all(rs_buf.at[k], ag_recv.at[k])
        rows = pl.ds(pl.multiple_of(k * rows_col + core * half, half), half)
        columns = pl.ds(pl.multiple_of(z * width, width), width)
        readings = [full[k, b].reshape(rows_half, deep) for b in range(2)]
        for h in range(2):
            summed = jnp.dot(readings[0], temps_ref[h, :deep, :], preferred_element_type=jnp.float32)
            summed += jnp.dot(readings[1], temps_ref[h, deep:, :], preferred_element_type=jnp.float32)
            rounded = (summed * scale).astype(jnp.bfloat16)
            out_buf[k, h * n_col:(h + 1) * n_col] = rounded.reshape(n_col, half, width)
            for e in [*range(n_half), *range(n_half + 1, n_col)]:
                peer = out_peer(e)
                pltpu.make_async_remote_copy(
                    out_buf.at[k, h * n_col + peer], out_ref.at[rows, columns], o_send.at[k], o_recv.at[k],
                    device_id=(chip * 2 + h, peer), device_id_type=MESH,
                ).start()
        pltpu.make_async_remote_copy(
            out_buf.at[k, other * n_col + z], out_ref.at[rows, columns], o_send.at[k], o_recv.at[k],
            device_id=partner, device_id_type=MESH,
        ).start()
        out_ref[rows, columns] = out_buf[k, core * n_col + z]

    load.wait()
    select(0)
    pl.semaphore_wait(barrier, greeted)
    start_core(0)
    for k in range(1, n_chunk):
        select(k)
        start_core(k)
        start_rs(k - 1)
    pltpu.make_async_remote_copy(
        temps_ref.at[core], temps_ref.at[core], x_send, x_recv,
        device_id=partner, device_id_type=MESH,
    ).start()
    start_rs(n_chunk - 1)
    stages = (start_z, start_ag, start_out)
    due = [(at + 1.05 * k, late, k) for late, at in enumerate((0, 2.7, 6.5)) for k in range(n_chunk)]
    for _, late, k in sorted(due):
        stages[late](k)
    wait_all(temps_ref.at[core], x_send)
    for k in range(n_chunk):
        wait_all(out_buf.at[k, pl.ds(0, 2 * n_col - 1)], o_recv.at[k])
        wait_all(out_buf.at[k, pl.ds(0, 2 * n_col - 1)], o_send.at[k])
        wait_all(core_buf.at[k], c_send.at[k])
        wait_all(rs_buf.at[k], rs_send.at[k])
        wait_all(z_buf.at[k], z_send.at[k])
        wait_all(rs_buf.at[k], ag_send.at[k])


def body(n_row, n_col, temps, sensors):
    tiers, snaps, width = temps.shape
    sens = sensors.shape[1]
    depth = tiers * snaps
    n_chunk = sens // (SUB * n_row)
    n_chip = n_row // 2
    rows_out = sens // n_col
    rows_col = rows_out // n_chunk
    bf16 = jnp.bfloat16
    return pl.pallas_call(
        functools.partial(kernel, n_row, n_col, n_chunk, tiers),
        out_shape=pltpu.VMEM((rows_out, n_col * width), bf16),
        in_specs=[pl.BlockSpec(memory_space=pl.ANY), pl.BlockSpec(memory_space=pltpu.VMEM)],
        out_specs=pl.BlockSpec(memory_space=pltpu.VMEM),
        scratch_shapes=[
            pltpu.VMEM((2, depth, width), bf16),
            pltpu.VMEM((n_col, n_chunk, 2, rows_col // 2, tiers), jnp.int32),
            pltpu.VMEM((n_chunk, 2, 2, n_chip, SUB, depth // 2), bf16),
            pltpu.VMEM((n_chunk, 2, n_chip, SUB, depth // 2), bf16),
            pltpu.VMEM((n_chunk, 2, n_chip, SUB, depth // 2), bf16),
            pltpu.VMEM((n_chunk, 2 * n_chip - 1, SUB, depth // 2), bf16),
            pltpu.VMEM((n_chunk, SUB, depth // 2), bf16),
            pltpu.VMEM((n_chunk, n_col // 2 - 1, SUB, depth // 2), bf16),
            pltpu.VMEM((n_chunk, 2, n_chip, SUB, depth // 2), bf16),
            pltpu.VMEM((n_chunk, 2 * n_col, rows_col // 2, width), bf16),
        ] + [pltpu.SemaphoreType.DMA((n_chunk,))] * 10 + [pltpu.SemaphoreType.DMA] * 3,
        compiler_params=pltpu.CompilerParams(collective_id=0, has_side_effects=True),
    )(temps.reshape(depth, width), sensors)


def solution(mesh):
    placed = (P(None, None, ("row", "col")), P())
    return jax.shard_map(
        functools.partial(body, mesh.shape["row"], mesh.shape["col"]),
        mesh=mesh, in_specs=placed, out_specs=P("col", "row"), check_vma=False,
    )
```

```python
import functools

import jax
import numpy as np
import jax.numpy as jnp
from jax import lax
from jax.experimental import pallas as pl
from jax.experimental.pallas import tpu as pltpu
from jax.sharding import PartitionSpec as P

SUB = 16
MESH = pl.DeviceIdType.MESH


def kernel(
    n_row, n_col, n_chunk, tiers,
    temps_hbm, sens_hbm, out_ref,
    temps_ref, sens_ref, sens_t, part, core_buf, pair_sum, rs_buf, z_src, z_buf, full, out_buf,
    c_send, c_recv, rs_send, rs_recv, z_send, z_recv,
    ag_send, ag_recv, o_send, o_recv, t_sem, s_sem, x_send, x_recv, near,
):
    r = lax.axis_index("row")
    z = lax.axis_index("col")
    core, chip = lax.rem(r, 2), r // 2
    other = 1 - core
    pair, parity = z // 2, lax.rem(z, 2)
    n_chip, n_pair = n_row // 2, n_col // 2
    depth, width = temps_ref.shape[1:]
    snaps, deep = depth // tiers, depth // 2
    rows_col = out_ref.shape[0] // n_chunk
    half = rows_col // 2
    rows_half = n_chip * SUB
    scale = float(np.float32(1.0) / np.sqrt(np.float32(depth)))
    partner = (chip * 2 + other, z)

    bits = n_chip.bit_length() - 1
    levels = max(bits + 1, n_col - 2)
    cube = sorted(
        ((d, e) for d in range(n_chip) for e in range(2) if d or e),
        key=lambda peer: -peer[0].bit_count() - peer[1],
    )

    def flip(value, mask):
        for bit in range(bits):
            if mask >> bit & 1:
                value = value + (1 << bit) * (1 - 2 * lax.rem(value // (1 << bit), 2))
        return value

    def cube_peer(d, e):
        peer = flip(chip, d)
        side = lax.rem(parity + e, 2)
        return side, peer, (peer * 2 + core, pair * 2 + side)

    def far_peer(e):
        return lax.rem(z + 2 * e, n_col)

    load = pltpu.make_async_copy(temps_hbm, temps_ref.at[core], t_sem)
    load_sens = pltpu.make_async_copy(sens_hbm, sens_ref, s_sem)
    barrier = pltpu.get_barrier_semaphore()

    def greet(sem):
        pl.semaphore_signal(sem, inc=1, device_id=partner, device_id_type=MESH)
        for bit in range(bits):
            pl.semaphore_signal(sem, inc=1, device_id=(flip(chip, 1 << bit) * 2 + core, z), device_id_type=MESH)

        @pl.when(z > 0)
        def _():
            pl.semaphore_signal(sem, inc=1, device_id=(r, z - 1), device_id_type=MESH)

        @pl.when(z < n_col - 1)
        def _():
            pl.semaphore_signal(sem, inc=1, device_id=(r, z + 1), device_id_type=MESH)

    neighbours = bits + 1 + (z > 0).astype(jnp.int32) + (z < n_col - 1).astype(jnp.int32)

    load_sens.start()
    load.start()
    greet(barrier)

    first_pixel = (r * n_col + z) * width
    load_sens.wait()
    offsets = jnp.transpose(sens_ref[...] - first_pixel).reshape(n_col, n_chunk, 2, half, tiers)
    for k in range(n_chunk):
        for h in range(2):
            sens_t[k, h] = offsets[:, k, h]
    pixel_ids = lax.broadcasted_iota(jnp.int32, (2 * rows_half, width), 1)

    def wait_all(ref, sem):
        pltpu.make_async_copy(ref, ref, sem).wait()

    def select(k):
        mine = sens_t[k].reshape(2 * rows_half, tiers)
        for t in range(0, tiers, 2):
            two = []
            for u in (t, t + 1):
                hot = (pixel_ids == mine[:, u:u + 1]).astype(jnp.float32).astype(jnp.bfloat16)
                two.append(lax.dot_general(
                    hot, temps_ref[core, u * snaps:(u + 1) * snaps, :],
                    (((1,), (1,)), ((), ())), preferred_element_type=jnp.float32,
                ))
            both = jnp.concatenate(two, axis=1).astype(jnp.bfloat16)
            b, at = divmod(t * snaps, deep)
            part[k, :, b, :, :, at:at + 2 * snaps] = both.reshape(2, n_chip, SUB, 2 * snaps)

    def start_core(k):
        pltpu.make_async_remote_copy(
            part.at[k, other], core_buf.at[k], c_send.at[k], c_recv.at[k],
            device_id=partner, device_id_type=MESH,
        ).start()

    def start_rs(k):
        wait_all(core_buf.at[k], c_recv.at[k])
        pair_sum[k] = part[k, core] + core_buf[k]
        for slot, (d, e) in enumerate(cube):
            side, peer, device = cube_peer(d, e)
            pltpu.make_async_remote_copy(
                pair_sum.at[k, side, peer], rs_buf.at[k, slot], rs_send.at[k], rs_recv.at[k],
                device_id=device, device_id_type=MESH,
            ).start()

    def start_z(k):
        wait_all(rs_buf.at[k], rs_recv.at[k])
        total = pair_sum[k, parity, chip]
        for slot in range(len(cube)):
            total = total + rs_buf[k, slot]
        z_src[k] = total
        for e in range(1, n_pair):
            pltpu.make_async_remote_copy(
                z_src.at[k], z_buf.at[k, e - 1], z_send.at[k], z_recv.at[k],
                device_id=(r, far_peer(e)), device_id_type=MESH,
            ).start()

    def start_ag(k):
        wait_all(z_buf.at[k], z_recv.at[k])
        total = z_src[k]
        for e in range(n_pair - 1):
            total = total + z_buf[k, e]
        full[k, parity, chip] = total
        for d, e in cube:
            pltpu.make_async_remote_copy(
                full.at[k, parity, chip], full.at[k, parity, chip], ag_send.at[k], ag_recv.at[k],
                device_id=cube_peer(d, e)[2], device_id_type=MESH,
            ).start()

    n_half = n_col // 2
    side_z = z // n_half

    def out_peer(e):
        across = (1 - side_z) * n_half + lax.rem(z + e, n_half)
        beside = side_z * n_half + lax.rem(z + e, n_half)
        return across if e < n_half else beside

    def start_out(k):
        if k == 0:
            wait_all(temps_ref.at[other], x_recv)
        wait_all(rs_buf.at[k], ag_recv.at[k])
        rows = pl.ds(pl.multiple_of(k * rows_col + core * half, half), half)
        columns = pl.ds(pl.multiple_of(z * width, width), width)
        readings = [full[k, b].reshape(rows_half, deep) for b in range(2)]
        for h in range(2):
            summed = jnp.dot(readings[0], temps_ref[h, :deep, :], preferred_element_type=jnp.float32)
            summed += jnp.dot(readings[1], temps_ref[h, deep:, :], preferred_element_type=jnp.float32)
            rounded = (summed * scale).astype(jnp.bfloat16)
            out_buf[k, h * n_col:(h + 1) * n_col] = rounded.reshape(n_col, half, width)
            for e in [*range(n_half), *range(n_half + 1, n_col)]:
                peer = out_peer(e)
                pltpu.make_async_remote_copy(
                    out_buf.at[k, h * n_col + peer], out_ref.at[rows, columns], o_send.at[k], o_recv.at[k],
                    device_id=(chip * 2 + h, peer), device_id_type=MESH,
                ).start()
        pltpu.make_async_remote_copy(
            out_buf.at[k, other * n_col + z], out_ref.at[rows, columns], o_send.at[k], o_recv.at[k],
            device_id=partner, device_id_type=MESH,
        ).start()
        out_ref[rows, columns] = out_buf[k, core * n_col + z]

    load.wait()
    select(0)
    pl.semaphore_wait(barrier, neighbours)
    start_core(0)
    for level in range(levels - 1):
        greet(near.at[level])
        if level + 1 < n_chunk:
            select(level + 1)
            start_core(level + 1)
        pl.semaphore_wait(near.at[level], neighbours)
    start_rs(0)
    for k in range(min(levels, n_chunk), n_chunk):
        select(k)
        start_core(k)
    for k in range(1, n_chunk - 1):
        start_rs(k)
    pltpu.make_async_remote_copy(
        temps_ref.at[core], temps_ref.at[core], x_send, x_recv,
        device_id=partner, device_id_type=MESH,
    ).start()
    start_rs(n_chunk - 1)
    stages = (start_z, start_ag, start_out)
    due = [(at + 1.05 * k, late, k) for late, at in enumerate((0, 2.7, 6.5)) for k in range(n_chunk)]
    for _, late, k in sorted(due):
        stages[late](k)
    wait_all(temps_ref.at[core], x_send)
    for k in range(n_chunk):
        wait_all(out_buf.at[k, pl.ds(0, 2 * n_col - 1)], o_recv.at[k])
        wait_all(out_buf.at[k, pl.ds(0, 2 * n_col - 1)], o_send.at[k])
        wait_all(core_buf.at[k], c_send.at[k])
        wait_all(rs_buf.at[k], rs_send.at[k])
        wait_all(z_buf.at[k], z_send.at[k])
        wait_all(rs_buf.at[k], ag_send.at[k])


def body(n_row, n_col, temps, sensors):
    tiers, snaps, width = temps.shape
    sens = sensors.shape[1]
    depth = tiers * snaps
    n_chunk = sens // (SUB * n_row)
    n_chip = n_row // 2
    rows_out = sens // n_col
    rows_col = rows_out // n_chunk
    bf16 = jnp.bfloat16
    return pl.pallas_call(
        functools.partial(kernel, n_row, n_col, n_chunk, tiers),
        out_shape=pltpu.VMEM((rows_out, n_col * width), bf16),
        in_specs=[pl.BlockSpec(memory_space=pl.ANY)] * 2,
        out_specs=pl.BlockSpec(memory_space=pltpu.VMEM),
        scratch_shapes=[
            pltpu.VMEM((2, depth, width), bf16),
            pltpu.VMEM((tiers, sens), jnp.int32),
            pltpu.VMEM((n_chunk, 2, n_col, rows_col // 2, tiers), jnp.int32),
            pltpu.VMEM((n_chunk, 2, 2, n_chip, SUB, depth // 2), bf16),
            pltpu.VMEM((n_chunk, 2, n_chip, SUB, depth // 2), bf16),
            pltpu.VMEM((n_chunk, 2, n_chip, SUB, depth // 2), bf16),
            pltpu.VMEM((n_chunk, 2 * n_chip - 1, SUB, depth // 2), bf16),
            pltpu.VMEM((n_chunk, SUB, depth // 2), bf16),
            pltpu.VMEM((n_chunk, n_col // 2 - 1, SUB, depth // 2), bf16),
            pltpu.VMEM((n_chunk, 2, n_chip, SUB, depth // 2), bf16),
            pltpu.VMEM((n_chunk, 2 * n_col, rows_col // 2, width), bf16),
        ] + [pltpu.SemaphoreType.DMA((n_chunk,))] * 10 + [pltpu.SemaphoreType.DMA] * 4 + [
            pltpu.SemaphoreType.REGULAR((max(n_chip.bit_length(), n_col - 2) - 1,)),
        ],
        compiler_params=pltpu.CompilerParams(collective_id=0, has_side_effects=True),
    )(temps.reshape(depth, width), sensors)


def solution(mesh):
    placed = (P(None, None, ("row", "col")), P())
    return jax.shard_map(
        functools.partial(body, mesh.shape["row"], mesh.shape["col"]),
        mesh=mesh, in_specs=placed, out_specs=P("col", "row"), check_vma=False,
    )
```

```python
import functools

import jax
import numpy as np
import jax.numpy as jnp
from jax import lax
from jax.experimental import pallas as pl
from jax.experimental.pallas import tpu as pltpu
from jax.sharding import PartitionSpec as P

SUB = 8
PIECES = 8
FIRST = 5
EARLY = 2
UNITS = (2, 2, 2, 2)
Z_AG = 2.9
AG_OUT = 3.3
MESH = pl.DeviceIdType.MESH


def kernel(
    n_row, n_col, n_chunk, tiers,
    temps_hbm, sens_hbm, out_ref,
    temps_ref, sens_ref, sens_t, part, core_buf, pair_sum, rs_buf, z_src, z_buf, full, out_buf, ahead, ahead_buf, tally,
    c_send, c_recv, rs_send, rs_recv, z_send, z_recv,
    ag_send, ag_recv, o_send, o_recv, f_send, f_recv, g_send, g_recv, t_sem, s_sem, x_send, x_recv,
):
    r = lax.axis_index("row")
    z = lax.axis_index("col")
    core, chip = lax.rem(r, 2), r // 2
    other = 1 - core
    pair, parity = z // 2, lax.rem(z, 2)
    n_chip, n_pair = n_row // 2, n_col // 2
    depth, width = temps_ref.shape[1:]
    snaps, deep = depth // tiers, depth // 2
    rows_core = out_ref.shape[0] // 2
    half = rows_core // n_chunk
    first_unit = [sum(UNITS[:j]) for j in range(len(UNITS))]
    rows_half = n_chip * SUB
    n_half = n_col // 2
    side = z // n_half
    early = ahead.shape[2]
    mirror = n_col - 1 - z
    inner = (z == n_half - 1) | (z == n_half)
    slab = depth // PIECES
    scale = float(np.float32(1.0) / np.sqrt(np.float32(depth)))
    partner = (chip * 2 + other, z)

    bits = n_chip.bit_length() - 1
    cube = sorted(
        ((d, e) for d in range(n_chip) for e in range(2) if d or e),
        key=lambda peer: -peer[0].bit_count() - peer[1],
    )

    def flip(value, mask):
        for bit in range(bits):
            if mask >> bit & 1:
                value = value + (1 << bit) * (1 - 2 * lax.rem(value // (1 << bit), 2))
        return value

    def cube_peer(d, e):
        peer = flip(chip, d)
        side = lax.rem(parity + e, 2)
        return side, peer, (peer * 2 + core, pair * 2 + side)

    def far_peer(e):
        return lax.rem(z + 2 * e, n_col)

    load = pltpu.make_async_copy(temps_hbm, temps_ref.at[core], t_sem)
    load_sens = pltpu.make_async_copy(sens_hbm, sens_ref, s_sem)
    barrier = pltpu.get_barrier_semaphore()

    greeted = 0
    for d, e in cube:
        if d:
            pl.semaphore_signal(barrier, inc=1, device_id=cube_peer(d, e)[2], device_id_type=MESH)
            greeted += 1
    for h in range(2):
        for e in range(n_col):
            if h or e:
                device = (chip * 2 + lax.rem(core + h, 2), lax.rem(z + e, n_col))
                pl.semaphore_signal(barrier, inc=1, device_id=device, device_id_type=MESH)
                greeted += 1

    load_sens.start()
    load.start()

    first_pixel = (r * n_col + z) * width
    load_sens.wait()
    offsets = jnp.transpose(sens_ref[...] - first_pixel).reshape(n_col, 2, n_chunk, half, tiers)
    for k in range(n_chunk):
        for h in range(2):
            sens_t[k, h] = offsets[:, h, k]

    def wait_all(ref, sem):
        pltpu.make_async_copy(ref, ref, sem).wait()

    def units(j):
        return pl.ds(first_unit[j], UNITS[j])

    def select(j):
        rows = UNITS[j] * 2 * rows_half
        mine = sens_t[units(j)].reshape(rows, tiers)
        pixel_ids = lax.broadcasted_iota(jnp.int32, (rows, width), 1)
        for t in range(0, tiers, 2):
            two = []
            for u in (t, t + 1):
                hot = (pixel_ids == mine[:, u:u + 1]).astype(jnp.float32).astype(jnp.bfloat16)
                two.append(lax.dot_general(
                    hot, temps_ref[core, u * snaps:(u + 1) * snaps, :],
                    (((1,), (1,)), ((), ())), preferred_element_type=jnp.float32,
                ))
            both = jnp.concatenate(two, axis=1).astype(jnp.bfloat16)
            b, at = divmod(t * snaps, deep)
            part[units(j), :, b, :, :, at:at + 2 * snaps] = both.reshape(UNITS[j], 2, n_chip, SUB, 2 * snaps)

    def start_core(j):
        pltpu.make_async_remote_copy(
            part.at[units(j), other], core_buf.at[units(j)], c_send.at[j], c_recv.at[j],
            device_id=partner, device_id_type=MESH,
        ).start()

    def start_rs(j):
        k = units(j)
        wait_all(core_buf.at[k], c_recv.at[j])
        pair_sum[k] = part[k, core] + core_buf[k]
        for slot, (d, e) in enumerate(cube):
            member, peer, device = cube_peer(d, e)
            pltpu.make_async_remote_copy(
                pair_sum.at[k, member, peer], rs_buf.at[slot, k], rs_send.at[j], rs_recv.at[j],
                device_id=device, device_id_type=MESH,
            ).start()

    def start_z(j):
        k = units(j)
        wait_all(rs_buf.at[:, k], rs_recv.at[j])
        total = pair_sum[k, parity, chip]
        for slot in range(len(cube)):
            total = total + rs_buf[slot, k]
        z_src[k] = total
        for e in range(1, n_pair):
            pltpu.make_async_remote_copy(
                z_src.at[k], z_buf.at[e - 1, k], z_send.at[j], z_recv.at[j],
                device_id=(r, far_peer(e)), device_id_type=MESH,
            ).start()

    def start_ag(j):
        k = units(j)
        wait_all(z_buf.at[:, k], z_recv.at[j])
        total = z_src[k]
        for e in range(n_pair - 1):
            total = total + z_buf[e, k]
        full[k, parity, chip] = total
        for d, e in cube:
            mine = full.at[k, parity, chip]
            pltpu.make_async_remote_copy(
                mine, mine, ag_send.at[j], ag_recv.at[j], device_id=cube_peer(d, e)[2], device_id_type=MESH,
            ).start()

    def ahead_rows(batch):
        return pl.ds((0, FIRST * slab)[batch], (FIRST * slab, depth - FIRST * slab)[batch])

    def start_ahead(piece):
        batch = int(piece >= FIRST)
        rows = pl.ds(piece * slab, slab)

        @pl.when(inner)
        def _():
            pltpu.make_async_remote_copy(
                temps_ref.at[core, rows, pl.ds(0, early)], ahead.at[core, rows], f_send.at[batch], f_recv.at[batch],
                device_id=(r, mirror), device_id_type=MESH,
            ).start()

    def relay_ahead(batch):
        mine = ahead.at[core, ahead_rows(batch)]

        @pl.when(inner)
        def _():
            wait_all(mine, f_recv.at[batch])
            pltpu.make_async_remote_copy(
                mine, mine, g_send.at[batch], g_recv.at[batch], device_id=partner, device_id_type=MESH,
            ).start()

    def across(e):
        return jnp.where(side == 0, n_half + e, n_half - 1 - e)

    def beside(e):
        return side * n_half + lax.rem(z + e, n_half)

    def product(rows, weights):
        summed = jnp.dot(rows[0], weights[:deep, :], preferred_element_type=jnp.float32)
        summed += jnp.dot(rows[1], weights[deep:, :], preferred_element_type=jnp.float32)
        return (summed * scale).astype(jnp.bfloat16)

    def send_out(j, h, source, columns, peer):
        rows = pl.ds(pl.multiple_of(core * rows_core + first_unit[j] * half, half), UNITS[j] * half)
        pltpu.make_async_remote_copy(
            source, out_ref.at[rows, columns], o_send.at[j], o_recv.at[j],
            device_id=(chip * 2 + h, peer), device_id_type=MESH,
        ).start()

    def keep_out(j, source, columns):
        rows = pl.ds(pl.multiple_of(core * rows_core + first_unit[j] * half, half), UNITS[j] * half)
        out_ref[rows, columns] = source[...]

    def start_out(j):
        if j == 0:
            wait_all(temps_ref.at[other], x_recv)
        k = units(j)
        wait_all(rs_buf.at[:, k], ag_recv.at[j])
        rows = pl.ds(first_unit[j] * half, UNITS[j] * half)
        first = pl.multiple_of(z * width, width)
        readings = [full[k, b].reshape(UNITS[j] * rows_half, deep) for b in range(2)]
        for h in range(2):
            result = product(readings, temps_ref.at[h]).reshape(UNITS[j], n_col, half, width)
            for i in range(UNITS[j]):
                out_buf[h * n_col:(h + 1) * n_col, (first_unit[j] + i) * half:(first_unit[j] + i + 1) * half] = result[i]

        def send_beside():
            for e in range(1, n_half):
                for h in range(2):
                    send_out(j, h, out_buf.at[h * n_col + beside(e), rows], pl.ds(first, width), beside(e))

        @pl.when(inner)
        def _():
            for e in range(n_half):
                for h in range(2):
                    block = out_buf.at[h * n_col + across(e), rows, pl.ds(early, width - early)]
                    send_out(j, h, block, pl.ds(pl.multiple_of(first + early, 128), width - early), across(e))
            send_beside()

        @pl.when(jnp.logical_not(inner))
        def _():
            send_beside()
            for e in reversed(range(n_half)):
                for h in range(2):
                    send_out(j, h, out_buf.at[h * n_col + across(e), rows], pl.ds(first, width), across(e))

        send_out(j, other, out_buf.at[other * n_col + z, rows], pl.ds(first, width), z)
        keep_out(j, out_buf.at[core * n_col + z, rows], pl.ds(first, width))

    def start_near(j):
        @pl.when(inner)
        def _():
            if j == 0:
                for batch in range(2):
                    wait_all(ahead.at[other, ahead_rows(batch)], g_recv.at[batch])
            k = units(j)
            rows = pl.ds(first_unit[j] * half, UNITS[j] * half)
            columns = pl.ds(pl.multiple_of(mirror * width, width), early)
            readings = [full[k, b].reshape(UNITS[j], n_col, half, deep) for b in range(2)]
            readings = [
                jnp.where(side == 0, both[:, :n_half], both[:, n_half:]).reshape(UNITS[j] * n_half * half, deep)
                for both in readings
            ]
            for h in range(2):
                result = product(readings, ahead.at[h]).reshape(UNITS[j], n_half, half, early)
                for i in range(UNITS[j]):
                    ahead_buf[h * n_half:(h + 1) * n_half, (first_unit[j] + i) * half:(first_unit[j] + i + 1) * half] = result[i]
                for e in range(1, n_half):
                    member = lax.rem(z + e, n_half)
                    send_out(j, h, ahead_buf.at[h * n_half + member, rows], columns, side * n_half + member)
            member = lax.rem(z, n_half)
            send_out(j, other, ahead_buf.at[other * n_half + member, rows], columns, z)
            keep_out(j, ahead_buf.at[core * n_half + member, rows], columns)

    groups = len(UNITS)
    load.wait()
    select(0)
    pl.semaphore_wait(barrier, greeted)
    start_core(0)
    for piece in range(FIRST):
        start_ahead(piece)
    for j in range(1, groups):
        select(j)
        start_core(j)
        start_rs(j - 1)
    pltpu.make_async_remote_copy(
        temps_ref.at[core], temps_ref.at[core], x_send, x_recv,
        device_id=partner, device_id_type=MESH,
    ).start()
    start_rs(groups - 1)

    def rest_ahead(_):
        for piece in range(FIRST, PIECES):
            start_ahead(piece)

    due = []
    for j in range(groups):
        at = 0.53 * (first_unit[j] + UNITS[j])
        due += [(at, start_z, j), (at + Z_AG, start_ag, j), (at + Z_AG + AG_OUT, start_out, j)]
    last_z = 0.53 * n_chunk + 0.01
    due += [(last_z, rest_ahead, 0), (last_z + 0.1, relay_ahead, 0)]
    late = 0.53 * n_chunk + Z_AG + AG_OUT + 0.01
    due += [(late, relay_ahead, 1)]
    due += [(late + 0.02, start_near, j) for j in range(groups)]
    for _, stage, j in sorted(due, key=lambda item: item[0]):
        stage(j)
    wait_all(temps_ref.at[core], x_send)

    @pl.when(inner)
    def _():
        for batch in range(2):
            wait_all(ahead.at[core, ahead_rows(batch)], f_send.at[batch])
            wait_all(ahead.at[core, ahead_rows(batch)], g_send.at[batch])

    for j in range(groups):
        lanes = UNITS[j] * width // 128
        sent = (2 * n_col - 1) * lanes

        for sem in (o_recv, o_send):
            @pl.when(inner)
            def _():
                wait_all(tally.at[pl.ds(0, sent - UNITS[j] * early // 128)], sem.at[j])

            @pl.when(jnp.logical_not(inner))
            def _():
                wait_all(tally.at[pl.ds(0, sent)], sem.at[j])

        k = units(j)
        wait_all(core_buf.at[k], c_send.at[j])
        wait_all(rs_buf.at[:, k], rs_send.at[j])
        wait_all(z_buf.at[:, k], z_send.at[j])
        wait_all(rs_buf.at[:, k], ag_send.at[j])


def body(n_row, n_col, temps, sensors):
    tiers, snaps, width = temps.shape
    sens = sensors.shape[1]
    depth = tiers * snaps
    n_chunk = sens // (SUB * n_row)
    n_chip = n_row // 2
    rows_out = sens // n_col
    rows_core = rows_out // 2
    deep = depth // 2
    early = width * EARLY // 4 // 128 * 128
    bf16 = jnp.bfloat16
    return pl.pallas_call(
        functools.partial(kernel, n_row, n_col, n_chunk, tiers),
        out_shape=pltpu.VMEM((rows_out, n_col * width), bf16),
        in_specs=[pl.BlockSpec(memory_space=pl.ANY)] * 2,
        out_specs=pl.BlockSpec(memory_space=pltpu.VMEM),
        scratch_shapes=[
            pltpu.VMEM((2, depth, width), bf16),
            pltpu.VMEM((tiers, sens), jnp.int32),
            pltpu.VMEM((n_chunk, 2, n_col, rows_core // n_chunk, tiers), jnp.int32),
            pltpu.VMEM((n_chunk, 2, 2, n_chip, SUB, deep), bf16),
            pltpu.VMEM((n_chunk, 2, n_chip, SUB, deep), bf16),
            pltpu.VMEM((n_chunk, 2, n_chip, SUB, deep), bf16),
            pltpu.VMEM((2 * n_chip - 1, n_chunk, SUB, deep), bf16),
            pltpu.VMEM((n_chunk, SUB, deep), bf16),
            pltpu.VMEM((n_col // 2 - 1, n_chunk, SUB, deep), bf16),
            pltpu.VMEM((n_chunk, 2, n_chip, SUB, deep), bf16),
            pltpu.VMEM((2 * n_col, rows_core, width), bf16),
            pltpu.VMEM((2, depth, early), bf16),
            pltpu.VMEM((n_col, rows_core, early), bf16),
            pltpu.VMEM((2 * n_col * max(UNITS) * width // 128, rows_core // n_chunk, 128), bf16),
        ] + [pltpu.SemaphoreType.DMA((len(UNITS),))] * 10
        + [pltpu.SemaphoreType.DMA((2,))] * 4 + [pltpu.SemaphoreType.DMA] * 4,
        compiler_params=pltpu.CompilerParams(collective_id=0, has_side_effects=True),
    )(temps.reshape(depth, width), sensors)


def solution(mesh):
    placed = (P(None, None, ("row", "col")), P())
    return jax.shard_map(
        functools.partial(body, mesh.shape["row"], mesh.shape["col"]),
        mesh=mesh, in_specs=placed, out_specs=P("col", "row"), check_vma=False,
    )
```

```python
import functools

import jax
import numpy as np
import jax.numpy as jnp
from jax import lax
from jax.experimental import pallas as pl
from jax.experimental.pallas import tpu as pltpu
from jax.sharding import PartitionSpec as P

SUB = 8
PIECES = 16
FIRST = 10
EARLY = 2
UNITS = (2, 2, 2, 2)
Z_AG = 2.9
AG_OUT = 3.3
MESH = pl.DeviceIdType.MESH


def kernel(
    n_row, n_col, n_chunk, tiers,
    temps_hbm, sens_hbm, out_ref,
    temps_ref, sens_ref, sens_t, part, core_buf, pair_sum, rs_buf, z_src, z_buf, full, out_buf, ahead, ahead_buf, tally,
    c_send, c_recv, rs_send, rs_recv, z_send, z_recv,
    ag_send, ag_recv, o_send, o_recv, f_send, f_recv, g_send, g_recv, t_sem, s_sem, x_send, x_recv,
):
    r = lax.axis_index("row")
    z = lax.axis_index("col")
    core, chip = lax.rem(r, 2), r // 2
    other = 1 - core
    pair, parity = z // 2, lax.rem(z, 2)
    n_chip, n_pair = n_row // 2, n_col // 2
    depth, width = temps_ref.shape[1:]
    snaps, deep = depth // tiers, depth // 2
    rows_core = out_ref.shape[0] // 2
    half = rows_core // n_chunk
    first_unit = [sum(UNITS[:j]) for j in range(len(UNITS))]
    rows_half = n_chip * SUB
    n_half = n_col // 2
    side = z // n_half
    early = ahead.shape[2]
    mirror = n_col - 1 - z
    inner = (z == n_half - 1) | (z == n_half)
    slab = depth // PIECES
    scale = float(np.float32(1.0) / np.sqrt(np.float32(depth)))
    partner = (chip * 2 + other, z)

    bits = n_chip.bit_length() - 1
    cube = sorted(
        ((d, e) for d in range(n_chip) for e in range(2) if d or e),
        key=lambda peer: -peer[0].bit_count() - peer[1],
    )

    def flip(value, mask):
        for bit in range(bits):
            if mask >> bit & 1:
                value = value + (1 << bit) * (1 - 2 * lax.rem(value // (1 << bit), 2))
        return value

    def cube_peer(d, e):
        peer = flip(chip, d)
        side = lax.rem(parity + e, 2)
        return side, peer, (peer * 2 + core, pair * 2 + side)

    def far_peer(e):
        return lax.rem(z + 2 * e, n_col)

    load = pltpu.make_async_copy(temps_hbm, temps_ref.at[core], t_sem)
    load_sens = pltpu.make_async_copy(sens_hbm, sens_ref, s_sem)
    barrier = pltpu.get_barrier_semaphore()

    greeted = 0
    for d, e in cube:
        if d:
            pl.semaphore_signal(barrier, inc=1, device_id=cube_peer(d, e)[2], device_id_type=MESH)
            greeted += 1
    for h in range(2):
        for e in range(n_col):
            if h or e:
                device = (chip * 2 + lax.rem(core + h, 2), lax.rem(z + e, n_col))
                pl.semaphore_signal(barrier, inc=1, device_id=device, device_id_type=MESH)
                greeted += 1

    load_sens.start()
    load.start()

    first_pixel = (r * n_col + z) * width
    load_sens.wait()
    offsets = jnp.transpose(sens_ref[...] - first_pixel).reshape(n_col, 2, n_chunk, half, tiers)
    for k in range(n_chunk):
        for h in range(2):
            sens_t[k, h] = offsets[:, h, k]

    def wait_all(ref, sem):
        pltpu.make_async_copy(ref, ref, sem).wait()

    def units(j):
        return pl.ds(first_unit[j], UNITS[j])

    def select(j):
        rows = UNITS[j] * 2 * rows_half
        mine = sens_t[units(j)].reshape(rows, tiers)
        pixel_ids = lax.broadcasted_iota(jnp.int32, (rows, width), 1)
        for t in range(0, tiers, 2):
            two = []
            for u in (t, t + 1):
                hot = (pixel_ids == mine[:, u:u + 1]).astype(jnp.float32).astype(jnp.bfloat16)
                two.append(lax.dot_general(
                    hot, temps_ref[core, u * snaps:(u + 1) * snaps, :],
                    (((1,), (1,)), ((), ())), preferred_element_type=jnp.float32,
                ))
            both = jnp.concatenate(two, axis=1).astype(jnp.bfloat16)
            b, at = divmod(t * snaps, deep)
            part[units(j), :, b, :, :, at:at + 2 * snaps] = both.reshape(UNITS[j], 2, n_chip, SUB, 2 * snaps)

    def start_core(j):
        pltpu.make_async_remote_copy(
            part.at[units(j), other], core_buf.at[units(j)], c_send.at[j], c_recv.at[j],
            device_id=partner, device_id_type=MESH,
        ).start()

    def start_rs(j):
        k = units(j)
        wait_all(core_buf.at[k], c_recv.at[j])
        pair_sum[k] = part[k, core] + core_buf[k]
        for slot, (d, e) in enumerate(cube):
            member, peer, device = cube_peer(d, e)
            pltpu.make_async_remote_copy(
                pair_sum.at[k, member, peer], rs_buf.at[slot, k], rs_send.at[j], rs_recv.at[j],
                device_id=device, device_id_type=MESH,
            ).start()

    def start_z(j):
        k = units(j)
        wait_all(rs_buf.at[:, k], rs_recv.at[j])
        total = pair_sum[k, parity, chip]
        for slot in range(len(cube)):
            total = total + rs_buf[slot, k]
        z_src[k] = total
        for e in range(1, n_pair):
            pltpu.make_async_remote_copy(
                z_src.at[k], z_buf.at[e - 1, k], z_send.at[j], z_recv.at[j],
                device_id=(r, far_peer(e)), device_id_type=MESH,
            ).start()

    def start_ag(j):
        k = units(j)
        wait_all(z_buf.at[:, k], z_recv.at[j])
        total = z_src[k]
        for e in range(n_pair - 1):
            total = total + z_buf[e, k]
        full[k, parity, chip] = total
        for d, e in cube:
            mine = full.at[k, parity, chip]
            pltpu.make_async_remote_copy(
                mine, mine, ag_send.at[j], ag_recv.at[j], device_id=cube_peer(d, e)[2], device_id_type=MESH,
            ).start()

    def ahead_rows(batch):
        return pl.ds((0, FIRST * slab)[batch], (FIRST * slab, depth - FIRST * slab)[batch])

    def start_ahead(piece):
        batch = int(piece >= FIRST)
        rows = pl.ds(piece * slab, slab)

        @pl.when(inner)
        def _():
            pltpu.make_async_remote_copy(
                temps_ref.at[core, rows, pl.ds(0, early)], ahead.at[core, rows], f_send.at[batch], f_recv.at[batch],
                device_id=(r, mirror), device_id_type=MESH,
            ).start()

    def relay_ahead(batch):
        mine = ahead.at[core, ahead_rows(batch)]

        @pl.when(inner)
        def _():
            wait_all(mine, f_recv.at[batch])
            pltpu.make_async_remote_copy(
                mine, mine, g_send.at[batch], g_recv.at[batch], device_id=partner, device_id_type=MESH,
            ).start()

    def across(e):
        return jnp.where(side == 0, n_half + e, n_half - 1 - e)

    def beside(e):
        return side * n_half + lax.rem(z + e, n_half)

    def product(rows, weights):
        summed = jnp.dot(rows[0], weights[:deep, :], preferred_element_type=jnp.float32)
        summed += jnp.dot(rows[1], weights[deep:, :], preferred_element_type=jnp.float32)
        return (summed * scale).astype(jnp.bfloat16)

    def send_out(j, h, source, columns, peer):
        rows = pl.ds(pl.multiple_of(core * rows_core + first_unit[j] * half, half), UNITS[j] * half)
        pltpu.make_async_remote_copy(
            source, out_ref.at[rows, columns], o_send.at[j], o_recv.at[j],
            device_id=(chip * 2 + h, peer), device_id_type=MESH,
        ).start()

    def keep_out(j, source, columns):
        rows = pl.ds(pl.multiple_of(core * rows_core + first_unit[j] * half, half), UNITS[j] * half)
        out_ref[rows, columns] = source[...]

    def start_out(j):
        if j == 0:
            wait_all(temps_ref.at[other], x_recv)
        k = units(j)
        wait_all(rs_buf.at[:, k], ag_recv.at[j])
        rows = pl.ds(first_unit[j] * half, UNITS[j] * half)
        first = pl.multiple_of(z * width, width)
        readings = [full[k, b].reshape(UNITS[j] * rows_half, deep) for b in range(2)]
        for h in range(2):
            result = product(readings, temps_ref.at[h]).reshape(UNITS[j], n_col, half, width)
            for i in range(UNITS[j]):
                out_buf[h * n_col:(h + 1) * n_col, (first_unit[j] + i) * half:(first_unit[j] + i + 1) * half] = result[i]

        def send_beside():
            for e in range(1, n_half):
                for h in range(2):
                    send_out(j, h, out_buf.at[h * n_col + beside(e), rows], pl.ds(first, width), beside(e))

        @pl.when(inner)
        def _():
            for e in range(n_half):
                for h in range(2):
                    block = out_buf.at[h * n_col + across(e), rows, pl.ds(early, width - early)]
                    send_out(j, h, block, pl.ds(pl.multiple_of(first + early, 128), width - early), across(e))
            send_beside()

        @pl.when(jnp.logical_not(inner))
        def _():
            if j < len(UNITS) - 1:
                send_beside()
            for e in reversed(range(n_half)):
                for h in range(2):
                    send_out(j, h, out_buf.at[h * n_col + across(e), rows], pl.ds(first, width), across(e))
            if j == len(UNITS) - 1:
                send_beside()

        send_out(j, other, out_buf.at[other * n_col + z, rows], pl.ds(first, width), z)
        keep_out(j, out_buf.at[core * n_col + z, rows], pl.ds(first, width))

    def start_near(j):
        @pl.when(inner)
        def _():
            if j == 0:
                for batch in range(2):
                    wait_all(ahead.at[other, ahead_rows(batch)], g_recv.at[batch])
            k = units(j)
            rows = pl.ds(first_unit[j] * half, UNITS[j] * half)
            columns = pl.ds(pl.multiple_of(mirror * width, width), early)
            readings = [full[k, b].reshape(UNITS[j], n_col, half, deep) for b in range(2)]
            readings = [
                jnp.where(side == 0, both[:, :n_half], both[:, n_half:]).reshape(UNITS[j] * n_half * half, deep)
                for both in readings
            ]
            for h in range(2):
                result = product(readings, ahead.at[h]).reshape(UNITS[j], n_half, half, early)
                for i in range(UNITS[j]):
                    ahead_buf[h * n_half:(h + 1) * n_half, (first_unit[j] + i) * half:(first_unit[j] + i + 1) * half] = result[i]
                for e in range(1, n_half):
                    member = lax.rem(z + e, n_half)
                    send_out(j, h, ahead_buf.at[h * n_half + member, rows], columns, side * n_half + member)
            member = lax.rem(z, n_half)
            send_out(j, other, ahead_buf.at[other * n_half + member, rows], columns, z)
            keep_out(j, ahead_buf.at[core * n_half + member, rows], columns)

    groups = len(UNITS)
    load.wait()
    select(0)
    pl.semaphore_wait(barrier, greeted)
    start_core(0)
    for piece in range(FIRST):
        start_ahead(piece)
    for j in range(1, groups):
        select(j)
        start_core(j)
        if j == 1:
            pl.when(core == 1)(functools.partial(start_rs, 0))
        elif j == 2:
            pl.when(core == 0)(functools.partial(start_rs, 0))
            start_rs(1)
        else:
            start_rs(j - 1)
    pltpu.make_async_remote_copy(
        temps_ref.at[core], temps_ref.at[core], x_send, x_recv,
        device_id=partner, device_id_type=MESH,
    ).start()
    start_rs(groups - 1)

    def start_z_ahead(j):
        start_z(j)
        for piece in range(FIRST + j, FIRST + j + 1 if j < groups - 1 else PIECES):
            start_ahead(piece)

    due = []
    for j in range(groups):
        at = 0.53 * (first_unit[j] + UNITS[j])
        due += [(at, start_z_ahead, j), (at + Z_AG, start_ag, j), (at + Z_AG + AG_OUT, start_out, j)]
    last_z = 0.53 * n_chunk + 0.01
    due += [(last_z + 0.1, relay_ahead, 0)]
    late = 0.53 * n_chunk + Z_AG + AG_OUT + 0.01
    due += [(late - 0.02, relay_ahead, 1)]
    due += [(late + 0.02, start_near, j) for j in range(groups)]
    for _, stage, j in sorted(due, key=lambda item: item[0]):
        stage(j)
    wait_all(temps_ref.at[core], x_send)

    @pl.when(inner)
    def _():
        for batch in range(2):
            wait_all(ahead.at[core, ahead_rows(batch)], f_send.at[batch])
            wait_all(ahead.at[core, ahead_rows(batch)], g_send.at[batch])

    for j in range(groups):
        lanes = UNITS[j] * width // 128
        sent = (2 * n_col - 1) * lanes

        for sem in (o_recv, o_send):
            @pl.when(inner)
            def _():
                wait_all(tally.at[pl.ds(0, sent - UNITS[j] * early // 128)], sem.at[j])

            @pl.when(jnp.logical_not(inner))
            def _():
                wait_all(tally.at[pl.ds(0, sent)], sem.at[j])

        k = units(j)
        wait_all(core_buf.at[k], c_send.at[j])
        wait_all(rs_buf.at[:, k], rs_send.at[j])
        wait_all(z_buf.at[:, k], z_send.at[j])
        wait_all(rs_buf.at[:, k], ag_send.at[j])


def body(n_row, n_col, temps, sensors):
    tiers, snaps, width = temps.shape
    sens = sensors.shape[1]
    depth = tiers * snaps
    n_chunk = sens // (SUB * n_row)
    n_chip = n_row // 2
    rows_out = sens // n_col
    rows_core = rows_out // 2
    deep = depth // 2
    early = width * EARLY // 4 // 128 * 128
    bf16 = jnp.bfloat16
    return pl.pallas_call(
        functools.partial(kernel, n_row, n_col, n_chunk, tiers),
        out_shape=pltpu.VMEM((rows_out, n_col * width), bf16),
        in_specs=[pl.BlockSpec(memory_space=pl.ANY)] * 2,
        out_specs=pl.BlockSpec(memory_space=pltpu.VMEM),
        scratch_shapes=[
            pltpu.VMEM((2, depth, width), bf16),
            pltpu.VMEM((tiers, sens), jnp.int32),
            pltpu.VMEM((n_chunk, 2, n_col, rows_core // n_chunk, tiers), jnp.int32),
            pltpu.VMEM((n_chunk, 2, 2, n_chip, SUB, deep), bf16),
            pltpu.VMEM((n_chunk, 2, n_chip, SUB, deep), bf16),
            pltpu.VMEM((n_chunk, 2, n_chip, SUB, deep), bf16),
            pltpu.VMEM((2 * n_chip - 1, n_chunk, SUB, deep), bf16),
            pltpu.VMEM((n_chunk, SUB, deep), bf16),
            pltpu.VMEM((n_col // 2 - 1, n_chunk, SUB, deep), bf16),
            pltpu.VMEM((n_chunk, 2, n_chip, SUB, deep), bf16),
            pltpu.VMEM((2 * n_col, rows_core, width), bf16),
            pltpu.VMEM((2, depth, early), bf16),
            pltpu.VMEM((n_col, rows_core, early), bf16),
            pltpu.VMEM((2 * n_col * max(UNITS) * width // 128, rows_core // n_chunk, 128), bf16),
        ] + [pltpu.SemaphoreType.DMA((len(UNITS),))] * 10
        + [pltpu.SemaphoreType.DMA((2,))] * 4 + [pltpu.SemaphoreType.DMA] * 4,
        compiler_params=pltpu.CompilerParams(collective_id=0, has_side_effects=True),
    )(temps.reshape(depth, width), sensors)


def solution(mesh):
    placed = (P(None, None, ("row", "col")), P())
    return jax.shard_map(
        functools.partial(body, mesh.shape["row"], mesh.shape["col"]),
        mesh=mesh, in_specs=placed, out_specs=P("col", "row"), check_vma=False,
    )
```
